32 devices in a mesh: dp: 4 (over x, core), space: 8 (over z, y).
Axes of the slice: x: 2, y: 2, z: 4, core: 2. Of those that a mesh axis runs over, the one named last changes fastest.
Arguments:
- section_three: bfloat16 [4, 64, 128, 512], P('dp', 'space'), parts along dimension 0, may hold values from -6 to 6
- section_four: bfloat16 [4, 32, 64, 1024], P('dp', 'space'), parts along dimension 0, may hold values from -6 to 6
- section_five: bfloat16 [4, 16, 32, 2048], P('dp', 'space'), parts along dimension 0, may hold values from -6 to 6
- lateral_three: bfloat16 [512, 256], P('space'), may hold values from -0.25 to 0.25
- lateral_four: bfloat16 [1024, 256], P('space'), may hold values from -0.1875 to 0.1875
- lateral_five: bfloat16 [2048, 256], P('space'), may hold values from -0.125 to 0.125
- lateral_bias_three: float32 [256], replicated, may hold values from -3 to 3
- lateral_bias_four: float32 [256], replicated, may hold values from -3 to 3
- lateral_bias_five: float32 [256], replicated, may hold values from -3 to 3
- output_three: bfloat16 [3, 3, 256, 256], P(None, None, 'space'), may hold values from -0.125 to 0.125
- output_four: bfloat16 [3, 3, 256, 256], P(None, None, 'space'), may hold values from -0.125 to 0.125
- output_five: bfloat16 [3, 3, 256, 256], P(None, None, 'space'), may hold values from -0.125 to 0.125
- output_bias_three: float32 [256], replicated, may hold values from -3 to 3
- output_bias_four: float32 [256], replicated, may hold values from -3 to 3
- output_bias_five: float32 [256], replicated, may hold values from -3 to 3
Outputs:
- level_three: bfloat16 [4, 64, 128, 256], P('dp', 'space'), parts along dimension 0
- level_four: bfloat16 [4, 32, 64, 256], P('dp', 'space'), parts along dimension 0
- level_five: bfloat16 [4, 16, 32, 256], P('dp'), parts along dimension 0
- level_six: bfloat16 [4, 8, 16, 256], P('dp'), parts along dimension 0
The draws below stay inside these ranges and needn't reach their ends.
There are 4 independent parts, one for each index of `dp`. The reference program is written for one: setup_inputs(seed, part) draws one part's arguments, and reference() takes and returns one part's arrays. A program takes and returns all parts, laid end to end along the dimension named above; an argument that names none is the same for every part. Nothing has to cross between parts.
All inputs are finite; a program needn't handle non-finite values.
Results may differ from the reference program's by a relative error of at most 0.0095.
Values may be sent and summed in bfloat16 or wider, within the bound.
A program may use at most 64 MiB of HBM per device.

```python
import jax
import jax.numpy as jnp

C3 = 512
C4 = 1024
C5 = 2048
FD = 256
IMG = 1
W5 = 32
H5 = 16
H4 = 32
H3 = 64
W4 = 64
W3 = 128


def levels(own_key, shape, shards, low, high):
    gain, own = 1.0, jax.random.fold_in(own_key, 6)
    for dim, shards_of in shards:
        draws = jnp.exp(jax.random.uniform(jax.random.fold_in(own, dim), (shards_of,), jnp.float32, low / len(shards), high / len(shards)))
        gain = gain * jnp.repeat(draws, shape[dim] // shards_of).reshape([-1 if axis == dim else 1 for axis in range(len(shape))])
    return gain


def gaussian(key, shape, width, reach, split=(), dtype=jnp.bfloat16):
    values = width * jax.random.normal(key, shape, jnp.float32)
    if split:
        values = values * levels(key, shape, split, -0.22, 0.18)
    return jnp.clip(values, -reach, reach).astype(dtype)


def setup_inputs(seed: int = 0, part: int = 0) -> dict:
    key_of = jax.random.split(jax.random.key(seed), 16)
    part_keys = jax.random.split(jax.random.fold_in(key_of[15], part), 16)
    section_three = gaussian(part_keys[0], (IMG, H3, W3, C3), 1.0, 6.0, ((1, 8),))
    section_four = gaussian(part_keys[1], (IMG, H4, W4, C4), 1.0, 6.0, ((1, 8),))
    section_five = gaussian(part_keys[2], (IMG, H5, W5, C5), 1.0, 6.0, ((1, 8),))
    lateral_three = gaussian(key_of[3], (C3, FD), C3 ** -0.5, 0.25, ((0, 8),))
    lateral_four = gaussian(key_of[4], (C4, FD), C4 ** -0.5, 0.1875, ((0, 8),))
    lateral_five = gaussian(key_of[5], (C5, FD), C5 ** -0.5, 0.125, ((0, 8),))
    lateral_bias_three = gaussian(key_of[6], (FD,), 0.5, 3.0, (), jnp.float32)
    lateral_bias_four = gaussian(key_of[7], (FD,), 0.5, 3.0, (), jnp.float32)
    lateral_bias_five = gaussian(key_of[8], (FD,), 0.5, 3.0, (), jnp.float32)
    output_three = gaussian(key_of[9], (3, 3, FD, FD), (9 * FD) ** -0.5, 0.125, ((2, 8),))
    output_four = gaussian(key_of[10], (3, 3, FD, FD), (9 * FD) ** -0.5, 0.125, ((2, 8),))
    output_five = gaussian(key_of[11], (3, 3, FD, FD), (9 * FD) ** -0.5, 0.125, ((2, 8),))
    output_bias_three = gaussian(key_of[12], (FD,), 0.5, 3.0, (), jnp.float32)
    output_bias_four = gaussian(key_of[13], (FD,), 0.5, 3.0, (), jnp.float32)
    output_bias_five = gaussian(key_of[14], (FD,), 0.5, 3.0, (), jnp.float32)
    return dict(section_three=section_three, section_four=section_four, section_five=section_five, lateral_three=lateral_three, lateral_four=lateral_four, lateral_five=lateral_five, lateral_bias_three=lateral_bias_three, lateral_bias_four=lateral_bias_four, lateral_bias_five=lateral_bias_five, output_three=output_three, output_four=output_four, output_five=output_five, output_bias_three=output_bias_three, output_bias_four=output_bias_four, output_bias_five=output_bias_five)


def lateral(features, weight, offset):
    images, rows, columns, channels = features.shape
    summed = jnp.dot(features.reshape(-1, channels), weight, preferred_element_type=jnp.float32) + offset
    return summed.reshape(images, rows, columns, -1)


def enlarge(coarse):
    return jnp.repeat(jnp.repeat(coarse, 2, axis=1), 2, axis=2)


def conv_rows(padded, weight, offset):
    images, rows_in, columns, channels = padded.shape
    height = rows_in - 2
    framed = jnp.pad(padded, ((0, 0), (0, 0), (1, 1), (0, 0)))
    summed = jnp.zeros((images * height * columns, weight.shape[3]), jnp.float32)
    for row_off in range(3):
        for col_off in range(3):
            window = framed[:, row_off:row_off + height, col_off:col_off + columns, :].reshape(-1, channels)
            summed = summed + jnp.dot(window, weight[row_off, col_off], preferred_element_type=jnp.float32)
    return (summed + offset).reshape(images, height, columns, -1).astype(jnp.bfloat16)


def pad_rows(field):
    return jnp.pad(field, ((0, 0), (1, 1), (0, 0), (0, 0)))


def reference(section_three, section_four, section_five, lateral_three, lateral_four, lateral_five, lateral_bias_three, lateral_bias_four, lateral_bias_five, output_three, output_four, output_five, output_bias_three, output_bias_four, output_bias_five):
    merged_five = lateral(section_five, lateral_five, lateral_bias_five).astype(jnp.bfloat16)
    merged_four = (lateral(section_four, lateral_four, lateral_bias_four) + enlarge(merged_five).astype(jnp.float32)).astype(jnp.bfloat16)
    merged_three = (lateral(section_three, lateral_three, lateral_bias_three) + enlarge(merged_four).astype(jnp.float32)).astype(jnp.bfloat16)
    level_three = conv_rows(pad_rows(merged_three), output_three, output_bias_three)
    level_four = conv_rows(pad_rows(merged_four), output_four, output_bias_four)
    level_five = conv_rows(pad_rows(merged_five), output_five, output_bias_five)
    level_six = level_five[:, ::2, ::2, :]
    return (level_three, level_four, level_five, level_six)
```

```python
import functools

import jax
import jax.numpy as jnp
from jax import lax
from jax.experimental import pallas as pl
from jax.experimental.pallas import tpu as pltpu
from jax.sharding import PartitionSpec as P

F32, BF16 = jnp.float32, jnp.bfloat16
L5, L4, L3, O3, O5, O4 = range(6)


def ring_place(s, n):
    return s // 2 + (s % 2) * (n - 1 - 2 * (s // 2))


def ring_owner(place, n):
    r = (place + 2 * n) % n
    back = r // (n // 2)
    return (1 - back) * (2 * r) + back * (2 * (n - 1 - r) + 1)


def spread(coarse):
    pixels = coarse.shape[0]
    fine = lax.broadcasted_iota(jnp.int32, (2 * pixels, pixels), 0) // 2
    pick = (fine == lax.broadcasted_iota(jnp.int32, (2 * pixels, pixels), 1)).astype(BF16)
    return jnp.dot(pick, coarse, preferred_element_type=F32)


def conv_tile(frame, weight, bias, start, pixels, width):
    rows = jnp.concatenate(
        [frame[pl.ds(pl.multiple_of(start + a * width, 16), pixels), :] for a in range(3)], axis=1
    )
    depth = weight.shape[2]
    part = [
        jnp.dot(
            rows,
            weight[:, c].reshape(3 * depth, weight.shape[3]),
            preferred_element_type=F32,
        )
        for c in range(3)
    ]
    column = lax.broadcasted_iota(jnp.int32, (pixels, 1), 0) % width
    left = jnp.where(column == 0, 0.0, pltpu.roll(part[0], 1, 0))
    right = jnp.where(column == width - 1, 0.0, pltpu.roll(part[2], pixels - 1, 0))
    return part[1] + left + right + bias[...]


def conv(frame, weight, bias, out, rows, wid, tall, first=0):
    def tile(i, carry):
        start = pl.multiple_of(i * (tall * wid), 16)
        out[pl.ds(start, tall * wid), :] = conv_tile(
            frame, weight, bias, start, tall * wid, wid
        ).astype(BF16)
        return carry

    lax.fori_loop(first, rows // tall, tile, 0)


def shared(unit, parts, split):
    if not split:
        return 0
    return parts // 2 // unit * unit if unit > 1 else parts // 3


def schedule(hops, lent, halved, line):
    begin = (2.34, 0.36, 2.39, 5.66, 3.55, 2.90)
    pace = (2.10, 2.62, 2.56, 3.93, 4.11, 5.31)
    lag = (2.50, 4.29, 5.09, 6.74, 3.76, 6.04)
    settled, half_to_five, line_lag, three_to_conv, five_lag, swap = 1.21, 4.39, 6.36, 20.56, 16.95, 3.70
    events = []
    ready = []
    for a in range(6):
        events.append((begin[a], "push", a, 0, 0))
        for k in range(2):
            for step in range(1, hops[k] + 1):
                at = begin[a] + pace[a] * step
                events.append((at, "pull", a, k, step))
                if lent[a]:
                    events.append((at + lag[a], "mate", a, k, step))
        ready.append(begin[a] + pace[a] * hops[0] + (lag[a] if lent[a] else 0.0) + 0.001)
    five = ready[L5] + settled
    if halved:
        events += [(swap, "swap", 0, 0, 0), (five, "half", 5, 0, 0)]
        five += half_to_five
    four = max(five, ready[L4] + settled) + 0.01
    three = max(four, ready[L3] + settled) + 0.01
    events += [(five, "merge", 5, 0, 0), (four, "merge", 4, 0, 0), (three, "merge", 3, 0, 0)]
    events += [(five + line_lag + 0.01 * j, "line", j, 0, 0) for j in range(1, line)]
    late = max(three + three_to_conv, ready[O3])
    events.append((late, "conv", 3, 0, 0))
    events.append((max(late + 0.01, five + line_lag + 0.5, ready[O5] + five_lag), "conv", 5, 0, 0))
    return [e[1:] for e in sorted(events, key=lambda e: e[0])]


def kernel(
    n, dims, dps,
    s3, s4, s5, l3, l4, l5, hb3, hb4, hb5, o3, o4, o5, hc3, hc4, hc5,
    r3, r5, r6, m4, w_o4, ob4,
    v3, v4, v5, v5_mate, own5, out5, in5, w_l5, w_l4, w_l3, w_o3, w_o5,
    m3, m5, lb3, lb4, lb5, ob3, ob5,
    ring_send, ring_recv, mate_send, mate_recv, core_send, core_recv,
    line_send, line_recv, pair_send, pair_recv, swap_send, swap_recv,
    halo_send, halo_recv, load5_sem, local_sem,
):
    (rows3, wid3), (rows4, wid4), (rows5, wid5) = dims
    dp, s = lax.axis_index("dp"), lax.axis_index("space")
    core = dp % 2
    plane = (dp // 2) % 2
    partner = (dp + 1 - 2 * core, s)
    mate = (dp + 2 - 4 * plane, s)
    paired = dps % 4 == 0
    place = ring_place(s, n)
    sign = 1 - 2 * core
    hops = (n // 2, n - 1 - n // 2)
    turn = (sign, -sign)
    target = [(dp, ring_owner(place + turn[k], n)) for k in range(2)]
    above, below = (dp, (s + n - 1) % n), (dp, (s + 1) % n)

    full = (w_l5, w_l4, w_l3, w_o3, w_o5, w_o4)
    mine = (l5, l4, l3, o3, o5, o4)
    half = w_l5.shape[1] // 2

    barrier = pltpu.get_barrier_semaphore()
    friends = [*target, partner] + ([mate] if paired else [])
    for device in friends:
        pl.semaphore_signal(
            barrier, inc=1, device_id=device, device_id_type=pl.DeviceIdType.MESH
        )

    parts = [mine[a].shape[0] for a in range(3)] + [3] * 3
    lent = [shared(16 if a < 3 else 1, parts[a], paired) for a in range(6)]
    halved = v5.shape[0] == 2
    if halved:
        parts[L5], lent[L5] = parts[L5] // 2, 0

    def chunk(a, owner, side, first, count):
        cols = pl.ds(pl.multiple_of(side * half, half), half)
        if a < 3:
            return full[a].at[pl.ds(pl.multiple_of(owner * parts[a] + first, 16), count), cols]
        size = mine[a].shape[2]
        return full[a].at[
            pl.ds(first, count), :, pl.ds(pl.multiple_of(owner * size, size), size), cols
        ]

    def ring_part(a, owner):
        return chunk(a, owner, core, plane * lent[a], parts[a] - lent[a])

    def mate_part(a, owner, sender):
        return chunk(a, owner, core, sender * (parts[a] - lent[a]), lent[a])

    def own_whole(a):
        if a < 3:
            size = parts[a]
            return full[a].at[pl.ds(pl.multiple_of(s * size, size), size), :]
        size = mine[a].shape[2]
        return full[a].at[:, :, pl.ds(pl.multiple_of(s * size, size), size), :]

    def own_shard(a):
        if a == L5 and halved:
            return mine[a].at[pl.ds(pl.multiple_of(plane * parts[a], 16), parts[a]), :]
        return mine[a]

    def bulk(a, count, side):
        cols = pl.ds(pl.multiple_of(side * half, half), half)
        if a < 3:
            return full[a].at[pl.ds(0, (n - 1) * count), cols]
        return full[a].at[pl.ds(0, count), :, pl.ds(0, (n - 1) * mine[a].shape[2]), cols]

    local = [pltpu.make_async_copy(own_shard(a), own_whole(a), local_sem.at[a]) for a in range(6)]
    features = [
        pltpu.make_async_copy(src, dst, local_sem.at[6 + k])
        for k, (src, dst) in enumerate(((s4, v4), (s3, v3)))
    ]
    biases = [
        pltpu.make_async_copy(src, dst, local_sem.at[8 + k])
        for k, (src, dst) in enumerate(
            ((hb3, lb3), (hb4, lb4), (hb5, lb5), (hc3, ob3), (hc4, ob4), (hc5, ob5))
        )
    ]
    pieces = v5.shape[0]
    load5 = [
        pltpu.make_async_copy(s5.at[:, pl.ds(0, v5.shape[2])], v5.at[q], load5_sem.at[q])
        for q in range(pieces)
    ]
    for copy in local:
        copy.start()
    if halved:
        for q in range(2):
            for owner in range(n):
                pltpu.make_async_copy(
                    s5.at[:, pl.ds((2 * owner + q) * parts[L5], parts[L5])],
                    v5.at[q, :, pl.ds(owner * parts[L5], parts[L5])],
                    load5_sem.at[q],
                ).start()
    else:
        load5[0].start()
    for copy in features + biases:
        copy.start()

    zero5 = jnp.zeros((wid5, m5.shape[1]), BF16)
    m5[pl.ds(0, wid5), :] = zero5
    m5[pl.ds(m5.shape[0] - wid5, wid5), :] = zero5
    with jax.named_scope("meet"):
        pl.semaphore_wait(barrier, len(friends))

    def remote(src, dst, send, recv, device):
        return pltpu.make_async_remote_copy(
            src_ref=src, dst_ref=dst, send_sem=send, recv_sem=recv,
            device_id=device, device_id_type=pl.DeviceIdType.MESH,
        )

    def send(a, k, step, owner):
        if step <= hops[k]:
            spot = ring_part(a, owner)
            remote(spot, spot, ring_send.at[a], ring_recv.at[a, k, step - 1], target[k]).start()

    def cross(a, spot):
        remote(spot, spot, core_send.at[a], core_recv.at[a], partner).start()

    def push(a):
        local[a].wait()
        for k in range(2):
            send(a, k, 1, s)

    def pull(a, k, step):
        owner = ring_owner(place - turn[k] * step, n)
        spot = ring_part(a, owner)
        remote(spot, spot, ring_send.at[a], ring_recv.at[a, k, step - 1], target[k]).wait_recv()
        send(a, k, step + 1, owner)
        if lent[a]:
            gift = mate_part(a, owner, plane)
            remote(gift, gift, mate_send.at[a], mate_recv.at[a, k, step - 1], mate).start()
        cross(a, spot)

    def accept(a, k, step):
        owner = ring_owner(place - turn[k] * step, n)
        spot = mate_part(a, owner, 1 - plane)
        remote(spot, spot, mate_send.at[a], mate_recv.at[a, k, step - 1], mate).wait_recv()
        cross(a, spot)

    def settle(a):
        spot = bulk(a, parts[a], 1 - core)
        remote(spot, spot, core_send.at[a], core_recv.at[a], partner).wait_recv()

    def map_rows(owner):
        size = rows5 * wid5
        return m5.at[pl.ds(pl.multiple_of(wid5 + owner * size, 16), size), :]

    across = s + 1 - 2 * (s % 2)

    def line_copy(j, owner):
        spot = map_rows(owner)
        peer = (dp, (s + 2 * j) % n)
        return remote(spot, spot, line_send.at[j - 1], line_recv.at[j - 1], peer)

    def pair_copy(j, owner):
        spot = map_rows(owner)
        return remote(spot, spot, pair_send.at[j], pair_recv.at[j], (dp, across))

    def line_pull(j):
        owner = (s + n - 2 * j) % n
        line_copy(j, owner).wait_recv()
        pair_copy(j, owner).start()

    if halved:
        swap = remote(v5.at[1 - plane], v5_mate, swap_send.at[0], swap_recv.at[0], mate)
        partial = remote(out5, in5, swap_send.at[1], swap_recv.at[1], mate)

    def half_five():
        settle(L5)
        swap.wait_recv()
        rows = jnp.concatenate([v5[plane], v5_mate[...]], axis=0)
        sums = jnp.dot(rows, w_l5[...], preferred_element_type=F32)
        own5[...] = sums[: own5.shape[0]]
        out5[...] = sums[own5.shape[0] :]
        partial.start()

    here = pl.multiple_of(wid5 + s * (rows5 * wid5), 16)
    halos = []
    for k, (frame, rows, wid) in enumerate(((m4, rows4, wid4), (m3, rows3, wid3))):
        first, last = frame.at[pl.ds(wid, wid), :], frame.at[pl.ds(rows * wid, wid), :]
        top, bottom = frame.at[pl.ds(0, wid), :], frame.at[pl.ds((rows + 1) * wid, wid), :]
        halos.append((
            remote(last, top, halo_send.at[2 * k], halo_recv.at[2 * k], below),
            remote(first, bottom, halo_send.at[2 * k + 1], halo_recv.at[2 * k + 1], above),
        ))

    def start_halo(pair):
        @pl.when(s < n - 1)
        def _():
            pair[0].start()

        @pl.when(s > 0)
        def _():
            pair[1].start()

    def end_halo(pair, frame, rows, wid):
        @pl.when(s > 0)
        def _():
            pair[0].wait_recv()
            pair[1].wait_send()

        @pl.when(s < n - 1)
        def _():
            pair[1].wait_recv()
            pair[0].wait_send()

        zero = jnp.zeros((wid, frame.shape[1]), BF16)

        @pl.when(s == 0)
        def _():
            frame[pl.ds(0, wid), :] = zero

        @pl.when(s == n - 1)
        def _():
            frame[pl.ds((rows + 1) * wid, wid), :] = zero

    def merge(level):
        if level == 5:
            for copy in biases:
                copy.wait()
            if halved:
                partial.wait_recv()
                sums = own5[...] + in5[...]
            else:
                settle(L5)
                load5[0].wait()
                sums = jnp.dot(v5[0], w_l5[...], preferred_element_type=F32)
            m5[pl.ds(here, rows5 * wid5), :] = (sums + lb5[...]).astype(BF16)
            for j in range(1, n // 2):
                line_copy(j, s).start()
            pair_copy(0, s).start()
        elif level == 4:
            settle(L4)
            features[0].wait()
            for r in range(rows5):
                up = spread(m5[pl.ds(pl.multiple_of(here + r * wid5, 16), wid5), :])
                base = 2 * r * wid4
                lat = jnp.dot(v4[base : base + 2 * wid4, :], w_l4[...], preferred_element_type=F32)
                m4[wid4 + base : wid4 + base + 2 * wid4, :] = (
                    lat + lb4[...] + jnp.concatenate([up, up], axis=0)
                ).astype(BF16)
            start_halo(halos[0])
        else:
            settle(L3)
            features[1].wait()

            def coarse_row(r, carry):
                up = spread(m4[pl.ds(pl.multiple_of(wid4 + r * wid4, 16), wid4), :])
                base = pl.multiple_of(2 * r * wid3, 16)
                lat = jnp.dot(v3[pl.ds(base, 2 * wid3), :], w_l3[...], preferred_element_type=F32)
                m3[pl.ds(pl.multiple_of(wid3 + base, 16), 2 * wid3), :] = (
                    lat + lb3[...] + jnp.concatenate([up, up], axis=0)
                ).astype(BF16)
                return carry

            lax.fori_loop(0, rows4, coarse_row, 0)
            start_halo(halos[1])

    def smooth(level):
        if level == 3:
            settle(O3)
            end_halo(halos[1], m3, rows3, wid3)
            conv(m3, w_o3, ob3, r3, rows3, wid3, 4)
            return
        settle(O5)
        for j in range(n // 2):
            pair_copy(j, (across + n - 2 * j) % n).wait_recv()
        conv(m5, w_o5, ob5, r5, n * rows5, wid5, 16)
        few, many = r6.shape[0], r5.shape[0]
        pixel = lax.broadcasted_iota(jnp.int32, (few, many), 0)
        take = 2 * wid5 * (pixel // (wid5 // 2)) + 2 * (pixel % (wid5 // 2))
        pick = (take == lax.broadcasted_iota(jnp.int32, (few, many), 1)).astype(BF16)
        r6[...] = jnp.dot(pick, r5[...], preferred_element_type=F32).astype(BF16)

    def handle(kind, a, k, step):
        if kind == "push":
            push(a)
        elif kind == "pull":
            pull(a, k, step)
        elif kind == "mate":
            accept(a, k, step)
        elif kind == "swap":
            for copy in load5:
                copy.wait()
            swap.start()
        elif kind == "half":
            half_five()
        elif kind == "line":
            line_pull(a)
        elif kind == "merge":
            merge(a)
        else:
            smooth(a)

    for event in schedule(hops, lent, halved, n // 2):
        with jax.named_scope("_".join(map(str, event))):
            handle(*event)

    with jax.named_scope("last"):
        settle(O4)
        end_halo(halos[0], m4, rows4, wid4)
    for a in range(6):
        spot = bulk(a, parts[a] - lent[a], core)
        remote(spot, spot, ring_send.at[a], core_recv.at[a], partner).wait_send()
        if lent[a]:
            spot = bulk(a, lent[a], core)
            remote(spot, spot, mate_send.at[a], core_recv.at[a], partner).wait_send()
        spot = bulk(a, parts[a], core)
        remote(spot, spot, core_send.at[a], core_recv.at[a], partner).wait_send()
    for j in range(1, n // 2):
        line_copy(j, s).wait_send()
    for j in range(n // 2):
        pair_copy(j, s).wait_send()
    if halved:
        swap.wait_send()
        partial.wait_send()


def finish(dims, r3, r5, r6, m4, w_o4, ob4, y3, y4, y5, y6, r4, sems):
    (_, _), (rows4, wid4), _ = dims
    copies = [
        pltpu.make_async_copy(src, dst, sems.at[k])
        for k, (src, dst) in enumerate(((r3, y3), (r5, y5), (r6, y6)))
    ]
    for copy in copies:
        copy.start()
    conv(m4, w_o4, ob4, r4, rows4, wid4, rows4)
    copies.append(pltpu.make_async_copy(r4, y4, sems.at[3]))
    copies[3].start()
    for copy in copies:
        copy.wait()


def on_device(n, dps, *arrays):
    s3, s4, s5, l3, l4, l5, lb3, lb4, lb5, o3, o4, o5, ob3, ob4, ob5 = arrays
    dims = tuple(x.shape[1:3] for x in (s3, s4, s5))
    fd = l3.shape[1]
    (rows3, wid3), (rows4, wid4), (rows5, wid5) = dims
    flat = [x.reshape(-1, x.shape[3]) for x in (s3, s4, s5)]
    biases = [b.reshape(1, fd) for b in (lb3, lb4, lb5, ob3, ob4, ob5)]
    anywhere = pl.BlockSpec(memory_space=pl.ANY)
    near = pl.BlockSpec(memory_space=pltpu.VMEM)
    far = max(n // 2, 1)
    size5, wide5 = flat[2].shape
    deep5 = l5.shape[0]
    halved = dps % 4 == 0 and deep5 % 256 == 0
    split5 = 2 if halved else 1

    def array(*shape):
        return pltpu.VMEM(shape, BF16)

    def result(pixels):
        return jax.ShapeDtypeStruct((pixels, fd), BF16)

    dma = pltpu.SemaphoreType.DMA
    held = pl.pallas_call(
        functools.partial(kernel, n, dims, dps),
        out_shape=(
            array(rows3 * wid3, fd),
            array(n * rows5 * wid5, fd),
            array(n * rows5 * wid5 // 4, fd),
            array((rows4 + 2) * wid4, fd),
            array(3, 3, n * o4.shape[2], fd),
            pltpu.VMEM((1, fd), F32),
        ),
        in_specs=[anywhere] * 15,
        out_specs=(near,) * 6,
        scratch_shapes=[
            *(array(*x.shape) for x in flat[:2]),
            array(split5, size5, wide5 // split5),
            array(size5, wide5 // split5),
            *(pltpu.VMEM((size5, fd), F32) for _ in range(3)),
            array(n * deep5 // split5, fd),
            array(n * l4.shape[0], fd),
            array(n * l3.shape[0], fd),
            *(array(3, 3, n * x.shape[2], fd) for x in (o3, o5)),
            array((rows3 + 2) * wid3, fd),
            array((n * rows5 + 2) * wid5, fd),
            *(pltpu.VMEM((1, fd), F32) for _ in range(5)),
            dma((6,)),
            dma((6, 2, far)),
            dma((6,)),
            dma((6, 2, far)),
            dma((6,)),
            dma((6,)),
            dma((far,)),
            dma((far,)),
            dma((far,)),
            dma((far,)),
            dma((2,)),
            dma((2,)),
            dma((4,)),
            dma((4,)),
            dma((2,)),
            dma((14,)),
        ],
        compiler_params=pltpu.CompilerParams(
            collective_id=0, has_side_effects=True, vmem_limit_bytes=40 * 1024 * 1024
        ),
    )(*[
        pltpu.with_memory_space_constraint(x, pltpu.HBM)
        for x in (*flat, l3, l4, l5, *biases[:3], o3, o4, o5, *biases[3:])
    ])
    y3, y4, y5, y6 = pl.pallas_call(
        functools.partial(finish, dims),
        out_shape=(
            result(rows3 * wid3),
            result(rows4 * wid4),
            result(n * rows5 * wid5),
            result(n * rows5 * wid5 // 4),
        ),
        in_specs=[near] * 6,
        out_specs=(anywhere,) * 4,
        scratch_shapes=[array(rows4 * wid4, fd), dma((4,))],
        compiler_params=pltpu.CompilerParams(vmem_limit_bytes=32 * 1024 * 1024),
    )(*[pltpu.with_memory_space_constraint(x, pltpu.VMEM) for x in held])
    return (
        y3.reshape(1, rows3, wid3, fd),
        y4.reshape(1, rows4, wid4, fd),
        y5.reshape(1, n * rows5, wid5, fd),
        y6.reshape(1, n * rows5 // 2, wid5 // 2, fd),
    )


def solution(mesh):
    split, rows = P("dp", "space", None, None), P("space", None)
    taps = P(None, None, "space", None)
    whole = P("dp", None, None, None)
    return jax.shard_map(
        functools.partial(on_device, mesh.shape["space"], mesh.shape["dp"]),
        mesh=mesh,
        in_specs=(split,) * 3 + (rows,) * 3 + (P(),) * 3 + (taps,) * 3 + (P(),) * 3,
        out_specs=(split, split, whole, whole),
        check_vma=False,
    )
```

```python
import functools

import jax
import jax.numpy as jnp
from jax import lax
from jax.experimental import pallas as pl
from jax.experimental.pallas import tpu as pltpu
from jax.sharding import PartitionSpec as P

F32, BF16 = jnp.float32, jnp.bfloat16
L5, L4, L3, O3, O5, O4 = range(6)


def ring_place(s, n):
    return s // 2 + (s % 2) * (n - 1 - 2 * (s // 2))


def ring_owner(place, n):
    r = (place + 2 * n) % n
    back = r // (n // 2)
    return (1 - back) * (2 * r) + back * (2 * (n - 1 - r) + 1)


def spread(coarse):
    pixels = coarse.shape[0]
    fine = lax.broadcasted_iota(jnp.int32, (2 * pixels, pixels), 0) // 2
    pick = (fine == lax.broadcasted_iota(jnp.int32, (2 * pixels, pixels), 1)).astype(BF16)
    return jnp.dot(pick, coarse, preferred_element_type=F32)


def conv_tile(frame, weight, bias, start, pixels, width):
    rows = jnp.concatenate(
        [frame[pl.ds(pl.multiple_of(start + a * width, 16), pixels), :] for a in range(3)], axis=1
    )
    depth = weight.shape[2]
    part = [
        jnp.dot(
            rows,
            weight[:, c].reshape(3 * depth, weight.shape[3]),
            preferred_element_type=F32,
        )
        for c in range(3)
    ]
    column = lax.broadcasted_iota(jnp.int32, (pixels, 1), 0) % width
    left = jnp.where(column == 0, 0.0, pltpu.roll(part[0], 1, 0))
    right = jnp.where(column == width - 1, 0.0, pltpu.roll(part[2], pixels - 1, 0))
    return part[1] + left + right + bias[...]


def conv(frame, weight, bias, out, rows, wid, tall, first=0):
    def tile(i, carry):
        start = pl.multiple_of(i * (tall * wid), 16)
        out[pl.ds(start, tall * wid), :] = conv_tile(
            frame, weight, bias, start, tall * wid, wid
        ).astype(BF16)
        return carry

    lax.fori_loop(first, rows // tall, tile, 0)


def shared(unit, parts, split):
    if not split:
        return 0
    return parts // 2 // unit * unit if unit > 1 else parts // 3


PUSH, PULL, MATE, SWAP, HALF, PRE, MERGE, REST, LINE, CONV = range(10)
ORDER = (
    100, 0, 500, 400, 1111, 3000, 200, 1101, 1011, 1001, 1501, 300, 1102, 1411, 1201, 1112,
    1012, 1002, 1511, 1401, 1211, 1301, 1412, 1103, 1003, 1202, 1113, 1502, 2102, 1013, 1402,
    1302, 1212, 2401, 1104, 1311, 1004, 4000, 1203, 1303, 1512, 2103, 2104, 2101, 1503, 1312,
    1213, 1403, 5400, 1204, 6500, 6400, 5300, 1313, 1304, 1413, 2502, 6300, 1513, 1404, 2402,
    2303, 2301, 1504, 8200, 2302, 2304, 8300, 2501, 8100, 7300, 2503, 2403, 2404, 9300, 2504,
    9500,
)
ROWS = (O4,)
WHOLE = (L3,)


def schedule(hops, lent, halved, line):
    begin = (2.34, 0.36, 2.39, 5.66, 3.55, 2.90)
    pace = (2.10, 2.62, 2.56, 3.93, 4.11, 5.31)
    lag = (2.50, 4.29, 5.09, 6.74, 3.76, 6.04)
    settled, half_to_five, line_lag, three_to_conv = 1.21, 4.39, 6.36, 3.0
    timed = [(0.5, (SWAP, 0, 0, 0))]
    ready = []
    for a in range(6):
        timed.append((begin[a], (PUSH, a, 0, 0)))
        for k in range(2):
            for step in range(1, hops[k] + 1):
                at = begin[a] + pace[a] * step
                timed.append((at, (PULL, a, k, step)))
                if lent[a] and k == 0:
                    timed.append((at + lag[a], (MATE, a, 0, step)))
        ready.append(begin[a] + pace[a] * hops[0] + (lag[a] if lent[a] else 0.0) + 0.001)
    five = ready[L5] + settled
    if halved:
        timed.append((five, (HALF, 0, 0, 0)))
        five += half_to_five
    four = max(five, ready[L4] + settled) + 0.01
    three = max(four, ready[L3] + settled) + 0.01
    conv = max(three + three_to_conv, ready[O3])
    timed += [
        (ready[L4] + settled, (PRE, 4, 0, 0)),
        (ready[L3] + settled, (PRE, 3, 0, 0)),
        (five, (MERGE, 5, 0, 0)),
        (four, (MERGE, 4, 0, 0)),
        (three, (MERGE, 3, 0, 0)),
        (three + 0.001, (REST, 3, 0, 0)),
        (conv, (CONV, 3, 0, 0)),
        (max(conv, five + line_lag, ready[O5]) + 0.5, (CONV, 5, 0, 0)),
    ]
    timed += [(five + line_lag + 0.01 * j, (LINE, j, 0, 0)) for j in range(1, line)]
    events = [e for _, e in sorted(timed, key=lambda e: e[0])]
    tuned = [(c // 1000, c // 100 % 10, c // 10 % 10, c % 10) for c in ORDER]
    return tuned if sorted(tuned) == sorted(events) else events


def kernel(
    n, dims, dps,
    s3, s4, s5, l3, l4, l5, hb3, hb4, hb5, o3, o4, o5, hc3, hc4, hc5,
    r3, r4, r5, r6,
    v3, v4, v5, v5_mate, own5, out5, in5, w_l5, w_l4, w_l3, w_o3, w_o5, w_o4,
    m3, m4, m5, part3, part4, bias,
    sent, ring_recv, mate_recv, core_recv, map_sent, line_recv, pair_recv,
    swap_sent, partial_sent, swap_recv, halo_send, halo_recv, local_sem,
):
    (rows3, wid3), (rows4, wid4), (rows5, wid5) = dims
    dp, s = lax.axis_index("dp"), lax.axis_index("space")
    core = dp % 2
    plane = (dp // 2) % 2
    partner = (dp + 1 - 2 * core, s)
    mate = (dp + 2 - 4 * plane, s)
    paired = dps % 4 == 0
    place = ring_place(s, n)
    sign = 1 - 2 * core
    hops = (n // 2, n - 1 - n // 2)
    turn = (sign, -sign)
    target = [(dp, ring_owner(place + turn[k], n)) for k in range(2)]
    above, below = (dp, (s + n - 1) % n), (dp, (s + 1) % n)

    full = (w_l5, w_l4, w_l3, w_o3, w_o5, w_o4)
    mine = (l5, l4, l3, o3, o5, o4)
    half = w_l5.shape[1] // 2

    barrier = pltpu.get_barrier_semaphore()
    friends = [*target, partner] + ([mate] if paired else [])
    for device in friends:
        pl.semaphore_signal(
            barrier, inc=1, device_id=device, device_id_type=pl.DeviceIdType.MESH
        )

    size = o3.shape[2]
    by_rows = [False] * 3 + [size % 32 == 0 and a in ROWS for a in range(3, 6)]
    parts = [mine[a].shape[0] for a in range(3)] + [size if by_rows[a] else 3 for a in range(3, 6)]
    lent = [
        shared(16 if a < 3 or by_rows[a] else 1, parts[a], paired and a not in WHOLE) for a in range(6)
    ]
    halved = v5.shape[0] == 2
    if halved:
        parts[L5], lent[L5] = parts[L5] // 2, 0

    def chunk(a, owner, side, first, count):
        cols = pl.ds(pl.multiple_of(side * half, half), half)
        if a < 3:
            return full[a].at[pl.ds(pl.multiple_of(owner * parts[a] + first, 16), count), cols]
        if by_rows[a]:
            return full[a].at[
                :, :, pl.ds(pl.multiple_of(owner * size + first, 16), count), cols
            ]
        return full[a].at[
            pl.ds(first, count), :, pl.ds(pl.multiple_of(owner * size, size), size), cols
        ]

    def ring_part(a, owner):
        return chunk(a, owner, core, plane * lent[a], parts[a] - lent[a])

    def mate_part(a, owner, sender):
        return chunk(a, owner, core, sender * (parts[a] - lent[a]), lent[a])

    def own_whole(a):
        if a < 3:
            return full[a].at[pl.ds(pl.multiple_of(s * parts[a], parts[a]), parts[a]), :]
        return full[a].at[:, :, pl.ds(pl.multiple_of(s * size, size), size), :]

    def own_shard(a):
        if a == L5 and halved:
            return mine[a].at[pl.ds(pl.multiple_of(plane * parts[a], 16), parts[a]), :]
        return mine[a]

    def bulk(a, count, owners, cols):
        if a < 3:
            return full[a].at[pl.ds(0, owners * count), cols]
        if by_rows[a]:
            return full[a].at[:, :, pl.ds(0, owners * count), cols]
        return full[a].at[pl.ds(0, count), :, pl.ds(0, owners * size), cols]

    one_side, both_sides = pl.ds(0, half), pl.ds(0, 2 * half)

    local = [pltpu.make_async_copy(own_shard(a), own_whole(a), local_sem.at[a]) for a in range(6)]
    features = [
        pltpu.make_async_copy(src, dst, local_sem.at[6 + k])
        for k, (src, dst) in enumerate(((s4, v4), (s3, v3)))
    ]
    bias_rows = [
        pltpu.make_async_copy(src, bias.at[pl.ds(k, 1), :], local_sem.at[8 + k])
        for k, src in enumerate((hb3, hb4, hb5, hc3, hc4, hc5))
    ]
    load5 = [
        pltpu.make_async_copy(s5.at[:, pl.ds(0, v5.shape[2])], v5.at[q], local_sem.at[14 + q])
        for q in range(v5.shape[0])
    ]
    lb3, lb4, lb5, ob3, ob4, ob5 = (bias.at[pl.ds(k, 1), :] for k in range(6))
    for copy in local:
        copy.start()
    if halved:
        for q in range(2):
            for owner in range(n):
                pltpu.make_async_copy(
                    s5.at[:, pl.ds((2 * owner + q) * parts[L5], parts[L5])],
                    v5.at[q, :, pl.ds(owner * parts[L5], parts[L5])],
                    local_sem.at[14 + q],
                ).start()
    else:
        load5[0].start()
    for copy in features + bias_rows:
        copy.start()

    zero5 = jnp.zeros((wid5, m5.shape[1]), BF16)
    m5[pl.ds(0, wid5), :] = zero5
    m5[pl.ds(m5.shape[0] - wid5, wid5), :] = zero5
    with jax.named_scope("meet"):
        pl.semaphore_wait(barrier, len(friends))

    def remote(src, dst, send, recv, device):
        return pltpu.make_async_remote_copy(
            src_ref=src, dst_ref=dst, send_sem=send, recv_sem=recv,
            device_id=device, device_id_type=pl.DeviceIdType.MESH,
        )

    def send(a, k, step, owner):
        if step <= hops[k]:
            spot = ring_part(a, owner)
            remote(spot, spot, sent.at[a], ring_recv.at[a, k * hops[0] + step - 1], target[k]).start()

    def cross(a, spot):
        remote(spot, spot, sent.at[a], core_recv.at[a], partner).start()

    def push(a):
        local[a].wait()
        for k in range(2):
            send(a, k, 1, s)

    def pull(a, k, step):
        owner = ring_owner(place - turn[k] * step, n)
        spot = ring_part(a, owner)
        sem = ring_recv.at[a, k * hops[0] + step - 1]
        remote(spot, spot, sent.at[a], sem, target[k]).wait_recv()
        send(a, k, step + 1, owner)
        if lent[a]:
            gift = mate_part(a, owner, plane)
            remote(gift, gift, sent.at[a], mate_recv.at[a, step - 1], mate).start()
        cross(a, spot)

    def accept(a, step):
        both = [k for k in range(2) if step <= hops[k]]
        spot = bulk(a, lent[a], len(both), one_side)
        remote(spot, spot, sent.at[a], mate_recv.at[a, step - 1], mate).wait_recv()
        for k in both:
            owner = ring_owner(place - turn[k] * step, n)
            cross(a, mate_part(a, owner, 1 - plane))

    def settle(a):
        spot = bulk(a, parts[a], n - 1, one_side)
        remote(spot, spot, sent.at[a], core_recv.at[a], partner).wait_recv()

    def drain(arrays):
        for a in arrays:
            spot = bulk(a, parts[a], n - 1, both_sides)
            remote(spot, spot, sent.at[a], core_recv.at[a], partner).wait_send()

    def map_rows(owner):
        count = rows5 * wid5
        return m5.at[pl.ds(pl.multiple_of(wid5 + owner * count, 16), count), :]

    across = s + 1 - 2 * (s % 2)

    def line_copy(j, owner):
        spot = map_rows(owner)
        peer = (dp, (s + 2 * j) % n)
        return remote(spot, spot, map_sent, line_recv.at[j - 1], peer)

    def pair_copy(owner):
        spot = map_rows(owner)
        return remote(spot, spot, map_sent, pair_recv, (dp, across))

    def map_view(count):
        return m5.at[pl.ds(0, count * rows5 * wid5), :]

    def line_pull(j):
        owner = (s + n - 2 * j) % n
        line_copy(j, owner).wait_recv()
        pair_copy(owner).start()

    if halved:
        swap = remote(v5.at[1 - plane], v5_mate, swap_sent, swap_recv.at[0], mate)
        partial = remote(out5, in5, partial_sent, swap_recv.at[1], mate)

    def half_five():
        settle(L5)
        swap.wait_recv()
        rows = jnp.concatenate([v5[plane], v5_mate[...]], axis=0)
        sums = jnp.dot(rows, w_l5[...], preferred_element_type=F32)
        own5[...] = sums[: own5.shape[0]]
        out5[...] = sums[own5.shape[0] :]
        partial.start()

    here = pl.multiple_of(wid5 + s * (rows5 * wid5), 16)
    halos = []
    for k, (frame, rows, wid) in enumerate(((m4, rows4, wid4), (m3, rows3, wid3))):
        first, last = frame.at[pl.ds(wid, wid), :], frame.at[pl.ds(rows * wid, wid), :]
        top, bottom = frame.at[pl.ds(0, wid), :], frame.at[pl.ds((rows + 1) * wid, wid), :]
        halos.append((
            remote(last, top, halo_send.at[2 * k], halo_recv.at[2 * k], below),
            remote(first, bottom, halo_send.at[2 * k + 1], halo_recv.at[2 * k + 1], above),
        ))

    def start_halo(pair):
        @pl.when(s < n - 1)
        def _():
            pair[0].start()

        @pl.when(s > 0)
        def _():
            pair[1].start()

    def end_halo(pair, frame, rows, wid):
        @pl.when(s > 0)
        def _():
            pair[0].wait_recv()
            pair[1].wait_send()

        @pl.when(s < n - 1)
        def _():
            pair[1].wait_recv()
            pair[0].wait_send()

        zero = jnp.zeros((wid, frame.shape[1]), BF16)

        @pl.when(s == 0)
        def _():
            frame[pl.ds(0, wid), :] = zero

        @pl.when(s == n - 1)
        def _():
            frame[pl.ds((rows + 1) * wid, wid), :] = zero

    def prepare(level):
        if level == 4:
            settle(L4)
            features[0].wait()
            part4[...] = jnp.dot(v4[...], w_l4[...], preferred_element_type=F32) + lb4[...]
            return
        settle(L3)
        features[1].wait()
        tall = 2 * wid3

        def tile(i, carry):
            span = pl.ds(pl.multiple_of(i * tall, tall), tall)
            part3[span, :] = (
                jnp.dot(v3[span, :], w_l3[...], preferred_element_type=F32) + lb3[...]
            )
            return carry

        lax.fori_loop(0, rows4, tile, 0)

    def add_row(r, coarse, fine, part, wid):
        up = spread(coarse[pl.ds(pl.multiple_of(wid + r * wid, 16), wid), :])
        base = pl.multiple_of(4 * r * wid, 16)
        fine[pl.ds(pl.multiple_of(2 * wid + base, 16), 4 * wid), :] = (
            part[pl.ds(base, 4 * wid), :] + jnp.concatenate([up, up], axis=0)
        ).astype(BF16)

    def merge(level):
        if level == 5:
            if halved:
                partial.wait_recv()
                sums = own5[...] + in5[...]
            else:
                settle(L5)
                sums = jnp.dot(v5[0], w_l5[...], preferred_element_type=F32)
            m5[pl.ds(here, rows5 * wid5), :] = (sums + lb5[...]).astype(BF16)
            for j in range(1, n // 2):
                line_copy(j, s).start()
            pair_copy(s).start()
        elif level == 4:
            own_five = m5.at[pl.ds(pl.multiple_of(here - wid5, 16), (rows5 + 1) * wid5), :]
            for r in range(rows5):
                add_row(r, own_five, m4, part4, wid5)
            start_halo(halos[0])
        else:
            for r in sorted({0, rows4 - 1}):
                add_row(r, m4, m3, part3, wid4)
            start_halo(halos[1])

    def rest():
        def row(r, carry):
            add_row(r, m4, m3, part3, wid4)
            return carry

        lax.fori_loop(1, rows4 - 1, row, 0)

    def smooth(level):
        if level == 3:
            settle(O3)
            end_halo(halos[1], m3, rows3, wid3)
            conv(m3, w_o3, ob3, r3, rows3, wid3, 4)
            return
        if level == 4:
            settle(O4)
            end_halo(halos[0], m4, rows4, wid4)
            conv(m4, w_o4, ob4, r4, rows4, wid4, rows4)
            return
        settle(O5)
        spot = map_view(n // 2)
        remote(spot, spot, map_sent, pair_recv, (dp, across)).wait_recv()
        conv(m5, w_o5, ob5, r5, n * rows5, wid5, 16)
        few, many = r6.shape[0], r5.shape[0]
        pixel = lax.broadcasted_iota(jnp.int32, (few, many), 0)
        take = 2 * wid5 * (pixel // (wid5 // 2)) + 2 * (pixel % (wid5 // 2))
        pick = (take == lax.broadcasted_iota(jnp.int32, (few, many), 1)).astype(BF16)
        r6[...] = jnp.dot(pick, r5[...], preferred_element_type=F32).astype(BF16)

    def start_swap():
        for copy in load5 + bias_rows:
            copy.wait()
        if halved:
            swap.start()

    def handle(kind, a, k, step):
        if kind == PUSH:
            push(a)
        elif kind == PULL:
            pull(a, k, step)
        elif kind == MATE:
            accept(a, step)
        elif kind == SWAP:
            start_swap()
        elif kind == HALF:
            half_five()
        elif kind == PRE:
            prepare(a)
        elif kind == MERGE:
            merge(a)
        elif kind == REST:
            rest()
        elif kind == LINE:
            line_pull(a)
        else:
            smooth(a)

    def drain_maps():
        spot = map_view(n - 1)
        remote(spot, spot, map_sent, pair_recv, (dp, across)).wait_send()
        if halved:
            swap.wait_send()
            partial.wait_send()

    for event in schedule(hops, lent, halved, n // 2):
        if event[:2] == (CONV, 5):
            drain((L5, L4, L3))
        with jax.named_scope("_".join(map(str, event))):
            handle(*event)

    with jax.named_scope("drain_maps"):
        drain_maps()
    with jax.named_scope("last"):
        smooth(4)
    with jax.named_scope("drain"):
        drain((O3, O5, O4))


def finish(*refs):
    results, outputs, sems = refs[:4], refs[4:8], refs[8]
    copies = [
        pltpu.make_async_copy(src, dst, sems.at[k])
        for k, (src, dst) in enumerate(zip(results, outputs))
    ]
    for copy in copies:
        copy.start()
    for copy in copies:
        copy.wait()


def on_device(n, dps, *arrays):
    s3, s4, s5, l3, l4, l5, lb3, lb4, lb5, o3, o4, o5, ob3, ob4, ob5 = arrays
    dims = tuple(x.shape[1:3] for x in (s3, s4, s5))
    fd = l3.shape[1]
    (rows3, wid3), (rows4, wid4), (rows5, wid5) = dims
    flat = [x.reshape(-1, x.shape[3]) for x in (s3, s4, s5)]
    biases = [b.reshape(1, fd) for b in (lb3, lb4, lb5, ob3, ob4, ob5)]
    anywhere = pl.BlockSpec(memory_space=pl.ANY)
    near = pl.BlockSpec(memory_space=pltpu.VMEM)
    far = max(n // 2, 1)
    size5, wide5 = flat[2].shape
    deep5 = l5.shape[0]
    halved = dps % 4 == 0 and deep5 % 256 == 0
    split5 = 2 if halved else 1

    def array(*shape):
        return pltpu.VMEM(shape, BF16)

    def result(pixels):
        return jax.ShapeDtypeStruct((pixels, fd), BF16)

    dma = pltpu.SemaphoreType.DMA
    held = pl.pallas_call(
        functools.partial(kernel, n, dims, dps),
        out_shape=(
            array(rows3 * wid3, fd),
            array(rows4 * wid4, fd),
            array(n * rows5 * wid5, fd),
            array(n * rows5 * wid5 // 4, fd),
        ),
        in_specs=[anywhere] * 15,
        out_specs=(near,) * 4,
        scratch_shapes=[
            *(array(*x.shape) for x in flat[:2]),
            array(split5, size5, wide5 // split5),
            array(size5, wide5 // split5),
            *(pltpu.VMEM((size5, fd), F32) for _ in range(3)),
            array(n * deep5 // split5, fd),
            array(n * l4.shape[0], fd),
            array(n * l3.shape[0], fd),
            *(array(3, 3, n * x.shape[2], fd) for x in (o3, o5, o4)),
            array((rows3 + 2) * wid3, fd),
            array((rows4 + 2) * wid4, fd),
            array((n * rows5 + 2) * wid5, fd),
            pltpu.VMEM((rows3 * wid3, fd), F32),
            pltpu.VMEM((rows4 * wid4, fd), F32),
            pltpu.VMEM((6, fd), F32),
            dma((6,)),
            dma((6, n - 1)),
            dma((6, far)),
            dma((6,)),
            dma,
            dma((far,)),
            dma,
            dma,
            dma,
            dma((2,)),
            dma((4,)),
            dma((4,)),
            dma((16,)),
        ],
        compiler_params=pltpu.CompilerParams(
            collective_id=0, has_side_effects=True, vmem_limit_bytes=40 * 1024 * 1024
        ),
    )(*[
        pltpu.with_memory_space_constraint(x, pltpu.HBM)
        for x in (*flat, l3, l4, l5, *biases[:3], o3, o4, o5, *biases[3:])
    ])
    y3, y4, y5, y6 = pl.pallas_call(
        finish,
        out_shape=(
            result(rows3 * wid3),
            result(rows4 * wid4),
            result(n * rows5 * wid5),
            result(n * rows5 * wid5 // 4),
        ),
        in_specs=[near] * 4,
        out_specs=(anywhere,) * 4,
        scratch_shapes=[dma((4,))],
        compiler_params=pltpu.CompilerParams(vmem_limit_bytes=32 * 1024 * 1024),
    )(*[pltpu.with_memory_space_constraint(x, pltpu.VMEM) for x in held])
    return (
        y3.reshape(1, rows3, wid3, fd),
        y4.reshape(1, rows4, wid4, fd),
        y5.reshape(1, n * rows5, wid5, fd),
        y6.reshape(1, n * rows5 // 2, wid5 // 2, fd),
    )


def solution(mesh):
    split, rows = P("dp", "space", None, None), P("space", None)
    taps = P(None, None, "space", None)
    whole = P("dp", None, None, None)
    return jax.shard_map(
        functools.partial(on_device, mesh.shape["space"], mesh.shape["dp"]),
        mesh=mesh,
        in_specs=(split,) * 3 + (rows,) * 3 + (P(),) * 3 + (taps,) * 3 + (P(),) * 3,
        out_specs=(split, split, whole, whole),
        check_vma=False,
    )
```

```python
import functools

import jax
import jax.numpy as jnp
from jax import lax
from jax.experimental import pallas as pl
from jax.experimental.pallas import tpu as pltpu
from jax.sharding import PartitionSpec as P

F32, BF16 = jnp.float32, jnp.bfloat16
L5, L4, L3, O3, O5, O4 = range(6)


def ring_place(s, n):
    return s // 2 + (s % 2) * (n - 1 - 2 * (s // 2))


def ring_owner(place, n):
    r = (place + 2 * n) % n
    back = r // (n // 2)
    return (1 - back) * (2 * r) + back * (2 * (n - 1 - r) + 1)


def spread(coarse):
    pixels = coarse.shape[0]
    fine = lax.broadcasted_iota(jnp.int32, (2 * pixels, pixels), 0) // 2
    pick = (fine == lax.broadcasted_iota(jnp.int32, (2 * pixels, pixels), 1)).astype(BF16)
    return jnp.dot(pick, coarse, preferred_element_type=F32)


def conv_tile(frame, weight, bias, start, pixels, width):
    rows = jnp.concatenate(
        [frame[pl.ds(pl.multiple_of(start + a * width, 16), pixels), :] for a in range(3)], axis=1
    )
    depth = weight.shape[2]
    part = [
        jnp.dot(
            rows,
            weight[:, c].reshape(3 * depth, weight.shape[3]),
            preferred_element_type=F32,
        )
        for c in range(3)
    ]
    column = lax.broadcasted_iota(jnp.int32, (pixels, 1), 0) % width
    left = jnp.where(column == 0, 0.0, pltpu.roll(part[0], 1, 0))
    right = jnp.where(column == width - 1, 0.0, pltpu.roll(part[2], pixels - 1, 0))
    return part[1] + left + right + bias[...]


def conv(frame, weight, bias, out, rows, wid, tall, first=0):
    def tile(i, carry):
        start = pl.multiple_of(i * (tall * wid), 16)
        out[pl.ds(start, tall * wid), :] = conv_tile(
            frame, weight, bias, start, tall * wid, wid
        ).astype(BF16)
        return carry

    lax.fori_loop(first, rows // tall, tile, 0)


def shared(unit, parts, split):
    if not split:
        return 0
    return parts // 2 // unit * unit if unit > 1 else parts // 3


PUSH, PULL, MATE, SWAP, HALF, PRE, MERGE, REST, LINE, CONV = range(10)
ORDER = (
    100, 0, 200, 500, 300, 3000, 1101, 1001, 1201, 1011, 1111, 1511, 400, 1501, 1102, 1002,
    1012, 1112, 1301, 1401, 1512, 1103, 1211, 2501, 2101, 1003, 1502, 1013, 1202, 1311, 1113,
    2102, 1402, 1104, 1411, 1302, 1004, 1212, 4000, 1312, 1203, 1403, 1513, 1303, 2104, 2103,
    1412, 1503, 5400, 6500, 1213, 1204, 6400, 5300, 1413, 1313, 2302, 6300, 1304, 1404, 8300,
    2502, 8200, 8100, 2403, 2301, 2503, 1504, 2303, 2401, 2304, 7300, 2404, 2402, 9300, 2504,
    9500,
)
ROWS = (O4,)
WHOLE = (L3,)


def schedule(hops, lent, halved, line):
    begin = (2.34, 0.36, 2.39, 5.66, 3.55, 2.90)
    pace = (2.10, 2.62, 2.56, 3.93, 4.11, 5.31)
    lag = (2.50, 4.29, 5.09, 6.74, 3.76, 6.04)
    settled, half_to_five, line_lag, three_to_conv = 1.21, 4.39, 6.36, 3.0
    timed = [(0.5, (SWAP, 0, 0, 0))]
    ready = []
    for a in range(6):
        timed.append((begin[a], (PUSH, a, 0, 0)))
        for k in range(2):
            for step in range(1, hops[k] + 1):
                at = begin[a] + pace[a] * step
                timed.append((at, (PULL, a, k, step)))
                if lent[a] and k == 0:
                    timed.append((at + lag[a], (MATE, a, 0, step)))
        ready.append(begin[a] + pace[a] * hops[0] + (lag[a] if lent[a] else 0.0) + 0.001)
    five = ready[L5] + settled
    if halved:
        timed.append((five, (HALF, 0, 0, 0)))
        five += half_to_five
    four = max(five, ready[L4] + settled) + 0.01
    three = max(four, ready[L3] + settled) + 0.01
    conv = max(three + three_to_conv, ready[O3])
    timed += [
        (ready[L4] + settled, (PRE, 4, 0, 0)),
        (ready[L3] + settled, (PRE, 3, 0, 0)),
        (five, (MERGE, 5, 0, 0)),
        (four, (MERGE, 4, 0, 0)),
        (three, (MERGE, 3, 0, 0)),
        (three + 0.001, (REST, 3, 0, 0)),
        (conv, (CONV, 3, 0, 0)),
        (max(conv, five + line_lag, ready[O5]) + 0.5, (CONV, 5, 0, 0)),
    ]
    timed += [(five + line_lag + 0.01 * j, (LINE, j, 0, 0)) for j in range(1, line)]
    events = [e for _, e in sorted(timed, key=lambda e: e[0])]
    tuned = [(c // 1000, c // 100 % 10, c // 10 % 10, c % 10) for c in ORDER]
    return tuned if sorted(tuned) == sorted(events) else events


def kernel(
    n, dims, dps,
    s3, s4, s5, l3, l4, l5, hb3, hb4, hb5, o3, o4, o5, hc3, hc4, hc5,
    r3, r4, r5, r6,
    v3, v4, v5, v5_mate, own5, out5, in5, w_l5, w_l4, w_l3, w_o3, w_o5, w_o4,
    m3, m4, m5, part3, part4, bias,
    sent, ring_recv, mate_recv, core_recv, map_sent, line_recv, pair_recv,
    swap_sent, partial_sent, swap_recv, halo_send, halo_recv, local_sem,
):
    (rows3, wid3), (rows4, wid4), (rows5, wid5) = dims
    dp, s = lax.axis_index("dp"), lax.axis_index("space")
    core = dp % 2
    plane = (dp // 2) % 2
    partner = (dp + 1 - 2 * core, s)
    mate = (dp + 2 - 4 * plane, s)
    paired = dps % 4 == 0
    place = ring_place(s, n)
    sign = 1 - 2 * core
    hops = (n // 2, n - 1 - n // 2)
    turn = (sign, -sign)
    target = [(dp, ring_owner(place + turn[k], n)) for k in range(2)]
    above, below = (dp, (s + n - 1) % n), (dp, (s + 1) % n)

    full = (w_l5, w_l4, w_l3, w_o3, w_o5, w_o4)
    mine = (l5, l4, l3, o3, o5, o4)
    half = w_l5.shape[1] // 2

    barrier = pltpu.get_barrier_semaphore()
    friends = [*target, partner] + ([mate] if paired else [])
    for device in friends:
        pl.semaphore_signal(
            barrier, inc=1, device_id=device, device_id_type=pl.DeviceIdType.MESH
        )

    size = o3.shape[2]
    by_rows = [False] * 3 + [size % 32 == 0 and a in ROWS for a in range(3, 6)]
    parts = [mine[a].shape[0] for a in range(3)] + [size if by_rows[a] else 3 for a in range(3, 6)]
    lent = [
        shared(16 if a < 3 or by_rows[a] else 1, parts[a], paired and a not in WHOLE) for a in range(6)
    ]
    halved = v5.shape[0] == 2
    if halved:
        parts[L5], lent[L5] = parts[L5] // 2, 0

    def chunk(a, owner, side, first, count):
        cols = pl.ds(pl.multiple_of(side * half, half), half)
        if a < 3:
            return full[a].at[pl.ds(pl.multiple_of(owner * parts[a] + first, 16), count), cols]
        if by_rows[a]:
            return full[a].at[
                :, :, pl.ds(pl.multiple_of(owner * size + first, 16), count), cols
            ]
        return full[a].at[
            pl.ds(first, count), :, pl.ds(pl.multiple_of(owner * size, size), size), cols
        ]

    def ring_part(a, owner):
        return chunk(a, owner, core, plane * lent[a], parts[a] - lent[a])

    def mate_part(a, owner, sender):
        return chunk(a, owner, core, sender * (parts[a] - lent[a]), lent[a])

    def own_whole(a):
        if a < 3:
            return full[a].at[pl.ds(pl.multiple_of(s * parts[a], parts[a]), parts[a]), :]
        return full[a].at[:, :, pl.ds(pl.multiple_of(s * size, size), size), :]

    def own_shard(a):
        if a == L5 and halved:
            return mine[a].at[pl.ds(pl.multiple_of(plane * parts[a], 16), parts[a]), :]
        return mine[a]

    def bulk(a, count, owners, cols):
        if a < 3:
            return full[a].at[pl.ds(0, owners * count), cols]
        if by_rows[a]:
            return full[a].at[:, :, pl.ds(0, owners * count), cols]
        return full[a].at[pl.ds(0, count), :, pl.ds(0, owners * size), cols]

    one_side, both_sides = pl.ds(0, half), pl.ds(0, 2 * half)

    local = [pltpu.make_async_copy(own_shard(a), own_whole(a), local_sem.at[a]) for a in range(6)]
    features = [
        pltpu.make_async_copy(src, dst, local_sem.at[6 + k])
        for k, (src, dst) in enumerate(((s4, v4), (s3, v3)))
    ]
    bias_rows = [
        pltpu.make_async_copy(src, bias.at[pl.ds(k, 1), :], local_sem.at[8 + k])
        for k, src in enumerate((hb3, hb4, hb5, hc3, hc4, hc5))
    ]
    load5 = [
        pltpu.make_async_copy(s5.at[:, pl.ds(0, v5.shape[2])], v5.at[q], local_sem.at[14 + q])
        for q in range(v5.shape[0])
    ]
    lb3, lb4, lb5, ob3, ob4, ob5 = (bias.at[pl.ds(k, 1), :] for k in range(6))
    for copy in local:
        copy.start()
    if halved:
        for q in range(2):
            for owner in range(n):
                pltpu.make_async_copy(
                    s5.at[:, pl.ds((2 * owner + q) * parts[L5], parts[L5])],
                    v5.at[q, :, pl.ds(owner * parts[L5], parts[L5])],
                    local_sem.at[14 + q],
                ).start()
    else:
        load5[0].start()
    for copy in features + bias_rows:
        copy.start()

    zero5 = jnp.zeros((wid5, m5.shape[1]), BF16)
    m5[pl.ds(0, wid5), :] = zero5
    m5[pl.ds(m5.shape[0] - wid5, wid5), :] = zero5
    with jax.named_scope("meet"):
        pl.semaphore_wait(barrier, len(friends))

    def remote(src, dst, send, recv, device):
        return pltpu.make_async_remote_copy(
            src_ref=src, dst_ref=dst, send_sem=send, recv_sem=recv,
            device_id=device, device_id_type=pl.DeviceIdType.MESH,
        )

    def send(a, k, step, owner):
        if step <= hops[k]:
            spot = ring_part(a, owner)
            remote(spot, spot, sent.at[a], ring_recv.at[a, k * hops[0] + step - 1], target[k]).start()

    def cross(a, spot):
        remote(spot, spot, sent.at[a], core_recv.at[a], partner).start()

    def push(a):
        local[a].wait()
        for k in range(2):
            send(a, k, 1, s)

    def pull(a, k, step):
        owner = ring_owner(place - turn[k] * step, n)
        spot = ring_part(a, owner)
        sem = ring_recv.at[a, k * hops[0] + step - 1]
        remote(spot, spot, sent.at[a], sem, target[k]).wait_recv()
        send(a, k, step + 1, owner)
        if lent[a]:
            gift = mate_part(a, owner, plane)
            remote(gift, gift, sent.at[a], mate_recv.at[a, step - 1], mate).start()
        cross(a, spot)

    def accept(a, step):
        both = [k for k in range(2) if step <= hops[k]]
        spot = bulk(a, lent[a], len(both), one_side)
        remote(spot, spot, sent.at[a], mate_recv.at[a, step - 1], mate).wait_recv()
        for k in both:
            owner = ring_owner(place - turn[k] * step, n)
            cross(a, mate_part(a, owner, 1 - plane))

    def settle(a):
        spot = bulk(a, parts[a], n - 1, one_side)
        remote(spot, spot, sent.at[a], core_recv.at[a], partner).wait_recv()

    def drain(arrays):
        for a in arrays:
            spot = bulk(a, parts[a], n - 1, both_sides)
            remote(spot, spot, sent.at[a], core_recv.at[a], partner).wait_send()

    def map_rows(owner):
        count = rows5 * wid5
        return m5.at[pl.ds(pl.multiple_of(wid5 + owner * count, 16), count), :]

    across = s + 1 - 2 * (s % 2)

    def line_copy(j, owner):
        spot = map_rows(owner)
        peer = (dp, (s + 2 * j) % n)
        return remote(spot, spot, map_sent, line_recv.at[j - 1], peer)

    def pair_copy(owner):
        spot = map_rows(owner)
        return remote(spot, spot, map_sent, pair_recv, (dp, across))

    def map_view(count):
        return m5.at[pl.ds(0, count * rows5 * wid5), :]

    def line_pull(j):
        owner = (s + n - 2 * j) % n
        line_copy(j, owner).wait_recv()
        pair_copy(owner).start()

    if halved:
        swap = remote(v5.at[1 - plane], v5_mate, swap_sent, swap_recv.at[0], mate)
        partial = remote(out5, in5, partial_sent, swap_recv.at[1], mate)

    def half_five():
        settle(L5)
        swap.wait_recv()
        rows = jnp.concatenate([v5[plane], v5_mate[...]], axis=0)
        sums = jnp.dot(rows, w_l5[...], preferred_element_type=F32)
        own5[...] = sums[: own5.shape[0]]
        out5[...] = sums[own5.shape[0] :]
        partial.start()

    here = pl.multiple_of(wid5 + s * (rows5 * wid5), 16)
    halos = []
    for k, (frame, rows, wid) in enumerate(((m4, rows4, wid4), (m3, rows3, wid3))):
        first, last = frame.at[pl.ds(wid, wid), :], frame.at[pl.ds(rows * wid, wid), :]
        top, bottom = frame.at[pl.ds(0, wid), :], frame.at[pl.ds((rows + 1) * wid, wid), :]
        halos.append((
            remote(last, top, halo_send.at[2 * k], halo_recv.at[2 * k], below),
            remote(first, bottom, halo_send.at[2 * k + 1], halo_recv.at[2 * k + 1], above),
        ))

    def start_halo(pair):
        @pl.when(s < n - 1)
        def _():
            pair[0].start()

        @pl.when(s > 0)
        def _():
            pair[1].start()

    def end_halo(pair, frame, rows, wid):
        @pl.when(s > 0)
        def _():
            pair[0].wait_recv()
            pair[1].wait_send()

        @pl.when(s < n - 1)
        def _():
            pair[1].wait_recv()
            pair[0].wait_send()

        zero = jnp.zeros((wid, frame.shape[1]), BF16)

        @pl.when(s == 0)
        def _():
            frame[pl.ds(0, wid), :] = zero

        @pl.when(s == n - 1)
        def _():
            frame[pl.ds((rows + 1) * wid, wid), :] = zero

    def prepare(level):
        if level == 4:
            settle(L4)
            features[0].wait()
            part4[...] = jnp.dot(v4[...], w_l4[...], preferred_element_type=F32) + lb4[...]
            return
        settle(L3)
        features[1].wait()
        tall = 2 * wid3

        def tile(i, carry):
            span = pl.ds(pl.multiple_of(i * tall, tall), tall)
            part3[span, :] = (
                jnp.dot(v3[span, :], w_l3[...], preferred_element_type=F32) + lb3[...]
            )
            return carry

        lax.fori_loop(0, rows4, tile, 0)

    def add_row(r, coarse, fine, part, wid):
        up = spread(coarse[pl.ds(pl.multiple_of(wid + r * wid, 16), wid), :])
        base = pl.multiple_of(4 * r * wid, 16)
        fine[pl.ds(pl.multiple_of(2 * wid + base, 16), 4 * wid), :] = (
            part[pl.ds(base, 4 * wid), :] + jnp.concatenate([up, up], axis=0)
        ).astype(BF16)

    def merge(level):
        if level == 5:
            if halved:
                partial.wait_recv()
                sums = own5[...] + in5[...]
            else:
                settle(L5)
                sums = jnp.dot(v5[0], w_l5[...], preferred_element_type=F32)
            m5[pl.ds(here, rows5 * wid5), :] = (sums + lb5[...]).astype(BF16)
            for j in range(1, n // 2):
                line_copy(j, s).start()
            pair_copy(s).start()
        elif level == 4:
            own_five = m5.at[pl.ds(pl.multiple_of(here - wid5, 16), (rows5 + 1) * wid5), :]
            for r in range(rows5):
                add_row(r, own_five, m4, part4, wid5)
            start_halo(halos[0])
        else:
            for r in sorted({0, rows4 - 1}):
                add_row(r, m4, m3, part3, wid4)
            start_halo(halos[1])

    def rest():
        def row(r, carry):
            add_row(r, m4, m3, part3, wid4)
            return carry

        lax.fori_loop(1, rows4 - 1, row, 0)

    def smooth(level):
        if level == 3:
            settle(O3)
            end_halo(halos[1], m3, rows3, wid3)
            conv(m3, w_o3, ob3, r3, rows3, wid3, 4)
            return
        if level == 4:
            settle(O4)
            end_halo(halos[0], m4, rows4, wid4)
            conv(m4, w_o4, ob4, r4, rows4, wid4, rows4)
            return
        settle(O5)
        spot = map_view(n // 2)
        remote(spot, spot, map_sent, pair_recv, (dp, across)).wait_recv()
        conv(m5, w_o5, ob5, r5, n * rows5, wid5, 16)
        few, many = r6.shape[0], r5.shape[0]
        pixel = lax.broadcasted_iota(jnp.int32, (few, many), 0)
        take = 2 * wid5 * (pixel // (wid5 // 2)) + 2 * (pixel % (wid5 // 2))
        pick = (take == lax.broadcasted_iota(jnp.int32, (few, many), 1)).astype(BF16)
        r6[...] = jnp.dot(pick, r5[...], preferred_element_type=F32).astype(BF16)

    def start_swap():
        for copy in load5 + bias_rows:
            copy.wait()
        if halved:
            swap.start()

    def handle(kind, a, k, step):
        if kind == PUSH:
            push(a)
        elif kind == PULL:
            pull(a, k, step)
        elif kind == MATE:
            accept(a, step)
        elif kind == SWAP:
            start_swap()
        elif kind == HALF:
            half_five()
        elif kind == PRE:
            prepare(a)
        elif kind == MERGE:
            merge(a)
        elif kind == REST:
            rest()
        elif kind == LINE:
            line_pull(a)
        else:
            smooth(a)

    def drain_maps():
        spot = map_view(n - 1)
        remote(spot, spot, map_sent, pair_recv, (dp, across)).wait_send()
        if halved:
            swap.wait_send()
            partial.wait_send()

    for event in schedule(hops, lent, halved, n // 2):
        if event[:2] == (CONV, 5):
            drain((L5, L4, L3))
        with jax.named_scope("_".join(map(str, event))):
            handle(*event)

    with jax.named_scope("drain_maps"):
        drain_maps()
    with jax.named_scope("last"):
        smooth(4)
    with jax.named_scope("drain"):
        drain((O3, O5, O4))


def finish(*refs):
    results, outputs, sems = refs[:4], refs[4:8], refs[8]
    copies = [
        pltpu.make_async_copy(src, dst, sems.at[k])
        for k, (src, dst) in enumerate(zip(results, outputs))
    ]
    for copy in copies:
        copy.start()
    for copy in copies:
        copy.wait()


def on_device(n, dps, *arrays):
    s3, s4, s5, l3, l4, l5, lb3, lb4, lb5, o3, o4, o5, ob3, ob4, ob5 = arrays
    dims = tuple(x.shape[1:3] for x in (s3, s4, s5))
    fd = l3.shape[1]
    (rows3, wid3), (rows4, wid4), (rows5, wid5) = dims
    flat = [x.reshape(-1, x.shape[3]) for x in (s3, s4, s5)]
    biases = [b.reshape(1, fd) for b in (lb3, lb4, lb5, ob3, ob4, ob5)]
    anywhere = pl.BlockSpec(memory_space=pl.ANY)
    near = pl.BlockSpec(memory_space=pltpu.VMEM)
    far = max(n // 2, 1)
    size5, wide5 = flat[2].shape
    deep5 = l5.shape[0]
    halved = dps % 4 == 0 and deep5 % 256 == 0
    split5 = 2 if halved else 1

    def array(*shape):
        return pltpu.VMEM(shape, BF16)

    def result(pixels):
        return jax.ShapeDtypeStruct((pixels, fd), BF16)

    dma = pltpu.SemaphoreType.DMA
    held = pl.pallas_call(
        functools.partial(kernel, n, dims, dps),
        out_shape=(
            array(rows3 * wid3, fd),
            array(rows4 * wid4, fd),
            array(n * rows5 * wid5, fd),
            array(n * rows5 * wid5 // 4, fd),
        ),
        in_specs=[anywhere] * 15,
        out_specs=(near,) * 4,
        scratch_shapes=[
            *(array(*x.shape) for x in flat[:2]),
            array(split5, size5, wide5 // split5),
            array(size5, wide5 // split5),
            *(pltpu.VMEM((size5, fd), F32) for _ in range(3)),
            array(n * deep5 // split5, fd),
            array(n * l4.shape[0], fd),
            array(n * l3.shape[0], fd),
            *(array(3, 3, n * x.shape[2], fd) for x in (o3, o5, o4)),
            array((rows3 + 2) * wid3, fd),
            array((rows4 + 2) * wid4, fd),
            array((n * rows5 + 2) * wid5, fd),
            pltpu.VMEM((rows3 * wid3, fd), F32),
            pltpu.VMEM((rows4 * wid4, fd), F32),
            pltpu.VMEM((6, fd), F32),
            dma((6,)),
            dma((6, n - 1)),
            dma((6, far)),
            dma((6,)),
            dma,
            dma((far,)),
            dma,
            dma,
            dma,
            dma((2,)),
            dma((4,)),
            dma((4,)),
            dma((16,)),
        ],
        compiler_params=pltpu.CompilerParams(
            collective_id=0, has_side_effects=True, vmem_limit_bytes=40 * 1024 * 1024
        ),
    )(*[
        pltpu.with_memory_space_constraint(x, pltpu.HBM)
        for x in (*flat, l3, l4, l5, *biases[:3], o3, o4, o5, *biases[3:])
    ])
    y3, y4, y5, y6 = pl.pallas_call(
        finish,
        out_shape=(
            result(rows3 * wid3),
            result(rows4 * wid4),
            result(n * rows5 * wid5),
            result(n * rows5 * wid5 // 4),
        ),
        in_specs=[near] * 4,
        out_specs=(anywhere,) * 4,
        scratch_shapes=[dma((4,))],
        compiler_params=pltpu.CompilerParams(vmem_limit_bytes=32 * 1024 * 1024),
    )(*[pltpu.with_memory_space_constraint(x, pltpu.VMEM) for x in held])
    return (
        y3.reshape(1, rows3, wid3, fd),
        y4.reshape(1, rows4, wid4, fd),
        y5.reshape(1, n * rows5, wid5, fd),
        y6.reshape(1, n * rows5 // 2, wid5 // 2, fd),
    )


def solution(mesh):
    split, rows = P("dp", "space", None, None), P("space", None)
    taps = P(None, None, "space", None)
    whole = P("dp", None, None, None)
    return jax.shard_map(
        functools.partial(on_device, mesh.shape["space"], mesh.shape["dp"]),
        mesh=mesh,
        in_specs=(split,) * 3 + (rows,) * 3 + (P(),) * 3 + (taps,) * 3 + (P(),) * 3,
        out_specs=(split, split, whole, whole),
        check_vma=False,
    )
```

```python
import functools

import jax
import jax.numpy as jnp
from jax import lax
from jax.experimental import pallas as pl
from jax.experimental.pallas import tpu as pltpu
from jax.sharding import PartitionSpec as P

F32, BF16 = jnp.float32, jnp.bfloat16
L5, L4, L3, O3, O5, O4 = range(6)


def ring_place(s, n):
    return s // 2 + (s % 2) * (n - 1 - 2 * (s // 2))


def ring_owner(place, n):
    r = (place + 2 * n) % n
    back = r // (n // 2)
    return (1 - back) * (2 * r) + back * (2 * (n - 1 - r) + 1)


def spread(coarse):
    pixels = coarse.shape[0]
    fine = lax.broadcasted_iota(jnp.int32, (2 * pixels, pixels), 0) // 2
    pick = (fine == lax.broadcasted_iota(jnp.int32, (2 * pixels, pixels), 1)).astype(BF16)
    return jnp.dot(pick, coarse, preferred_element_type=F32)


def conv_tile(frame, weight, bias, start, pixels, width):
    rows = jnp.concatenate(
        [frame[pl.ds(pl.multiple_of(start + a * width, 16), pixels), :] for a in range(3)], axis=1
    )
    depth = weight.shape[2]
    part = [
        jnp.dot(
            rows,
            weight[:, c].reshape(3 * depth, weight.shape[3]),
            preferred_element_type=F32,
        )
        for c in range(3)
    ]
    column = lax.broadcasted_iota(jnp.int32, (pixels, 1), 0) % width
    left = jnp.where(column == 0, 0.0, pltpu.roll(part[0], 1, 0))
    right = jnp.where(column == width - 1, 0.0, pltpu.roll(part[2], pixels - 1, 0))
    return part[1] + left + right + bias[...]


def conv(frame, weight, bias, out, rows, wid, tall, first=0):
    def tile(i, carry):
        start = pl.multiple_of(i * (tall * wid), 16)
        out[pl.ds(start, tall * wid), :] = conv_tile(
            frame, weight, bias, start, tall * wid, wid
        ).astype(BF16)
        return carry

    lax.fori_loop(first, rows // tall, tile, 0)


def shared(unit, parts, split):
    if not split:
        return 0
    return parts // 2 // unit * unit if unit > 1 else parts // 3


PUSH, PULL, MATE, SWAP, HALF, PRE, MERGE, REST, LINE, CONV = range(10)
ORDER = (
    100, 0, 200, 500, 300, 3000, 1101, 1001, 1201, 1011, 1111, 1511, 400, 1501, 1102, 1002,
    1012, 1112, 1301, 1401, 1512, 1103, 1211, 2501, 2101, 1003, 1502, 1013, 1202, 1311, 1113,
    2102, 1402, 1104, 1411, 1302, 1004, 1212, 4000, 1312, 1203, 1403, 1513, 1303, 2104, 2103,
    1412, 1503, 5400, 6500, 1213, 1204, 6400, 5300, 1413, 1313, 2302, 6300, 1304, 1404, 8300,
    2502, 8200, 8100, 2403, 2301, 2503, 1504, 2303, 2401, 2304, 7300, 2404, 2402, 9300, 2504,
    9500,
)
ROWS = (O4,)
WHOLE = (L3,)


def schedule(hops, lent, halved, line):
    begin = (2.34, 0.36, 2.39, 5.66, 3.55, 2.90)
    pace = (2.10, 2.62, 2.56, 3.93, 4.11, 5.31)
    lag = (2.50, 4.29, 5.09, 6.74, 3.76, 6.04)
    settled, half_to_five, line_lag, three_to_conv = 1.21, 4.39, 6.36, 3.0
    timed = [(0.5, (SWAP, 0, 0, 0))]
    ready = []
    for a in range(6):
        timed.append((begin[a], (PUSH, a, 0, 0)))
        for k in range(2):
            for step in range(1, hops[k] + 1):
                at = begin[a] + pace[a] * step
                timed.append((at, (PULL, a, k, step)))
                if lent[a] and k == 0:
                    timed.append((at + lag[a], (MATE, a, 0, step)))
        ready.append(begin[a] + pace[a] * hops[0] + (lag[a] if lent[a] else 0.0) + 0.001)
    five = ready[L5] + settled
    if halved:
        timed.append((five, (HALF, 0, 0, 0)))
        five += half_to_five
    four = max(five, ready[L4] + settled) + 0.01
    three = max(four, ready[L3] + settled) + 0.01
    conv = max(three + three_to_conv, ready[O3])
    timed += [
        (ready[L4] + settled, (PRE, 4, 0, 0)),
        (ready[L3] + settled, (PRE, 3, 0, 0)),
        (five, (MERGE, 5, 0, 0)),
        (four, (MERGE, 4, 0, 0)),
        (three, (MERGE, 3, 0, 0)),
        (three + 0.001, (REST, 3, 0, 0)),
        (conv, (CONV, 3, 0, 0)),
        (max(conv, five + line_lag, ready[O5]) + 0.5, (CONV, 5, 0, 0)),
    ]
    timed += [(five + line_lag + 0.01 * j, (LINE, j, 0, 0)) for j in range(1, line)]
    events = [e for _, e in sorted(timed, key=lambda e: e[0])]
    tuned = [(c // 1000, c // 100 % 10, c // 10 % 10, c % 10) for c in ORDER]
    return tuned if sorted(tuned) == sorted(events) else events


def kernel(
    n, dims, dps,
    s3, s4, s5, l3, l4, l5, hb3, hb4, hb5, o3, o4, o5, hc3, hc4, hc5,
    r3, r4, r5, r6,
    v3, v4, v5, v5_mate, own5, out5, in5, w_l5, w_l4, w_l3, w_o3, w_o5, w_o4,
    m3, m4, m5, part3, part4, bias,
    sent, ring_recv, mate_recv, core_recv, map_sent, line_recv, pair_recv,
    swap_sent, partial_sent, swap_recv, halo_send, halo_recv, local_sem,
):
    (rows3, wid3), (rows4, wid4), (rows5, wid5) = dims
    dp, s = lax.axis_index("dp"), lax.axis_index("space")
    core = dp % 2
    plane = (dp // 2) % 2
    partner = (dp + 1 - 2 * core, s)
    mate = (dp + 2 - 4 * plane, s)
    paired = dps % 4 == 0
    place = ring_place(s, n)
    sign = 1 - 2 * core
    hops = (n // 2, n - 1 - n // 2)
    turn = (sign, -sign)
    target = [(dp, ring_owner(place + turn[k], n)) for k in range(2)]
    above, below = (dp, (s + n - 1) % n), (dp, (s + 1) % n)

    full = (w_l5, w_l4, w_l3, w_o3, w_o5, w_o4)
    mine = (l5, l4, l3, o3, o5, o4)
    half = w_l5.shape[1] // 2

    barrier = pltpu.get_barrier_semaphore()
    friends = [*target, partner] + ([mate] if paired else [])
    for device in friends:
        pl.semaphore_signal(
            barrier, inc=1, device_id=device, device_id_type=pl.DeviceIdType.MESH
        )

    size = o3.shape[2]
    by_rows = [False] * 3 + [size % 32 == 0 and a in ROWS for a in range(3, 6)]
    parts = [mine[a].shape[0] for a in range(3)] + [size if by_rows[a] else 3 for a in range(3, 6)]
    lent = [
        shared(16 if a < 3 or by_rows[a] else 1, parts[a], paired and a not in WHOLE) for a in range(6)
    ]
    halved = v5.shape[0] == 2
    if halved:
        parts[L5], lent[L5] = parts[L5] // 2, 0

    def chunk(a, owner, side, first, count):
        cols = pl.ds(pl.multiple_of(side * half, half), half)
        if a < 3:
            return full[a].at[pl.ds(pl.multiple_of(owner * parts[a] + first, 16), count), cols]
        if by_rows[a]:
            return full[a].at[
                :, :, pl.ds(pl.multiple_of(owner * size + first, 16), count), cols
            ]
        return full[a].at[
            pl.ds(first, count), :, pl.ds(pl.multiple_of(owner * size, size), size), cols
        ]

    def ring_part(a, owner):
        return chunk(a, owner, core, plane * lent[a], parts[a] - lent[a])

    def mate_part(a, owner, sender):
        return chunk(a, owner, core, sender * (parts[a] - lent[a]), lent[a])

    def own_whole(a):
        if a < 3:
            return full[a].at[pl.ds(pl.multiple_of(s * parts[a], parts[a]), parts[a]), :]
        return full[a].at[:, :, pl.ds(pl.multiple_of(s * size, size), size), :]

    def own_shard(a):
        if a == L5 and halved:
            return mine[a].at[pl.ds(pl.multiple_of(plane * parts[a], 16), parts[a]), :]
        return mine[a]

    def bulk(a, count, owners, cols):
        if a < 3:
            return full[a].at[pl.ds(0, owners * count), cols]
        if by_rows[a]:
            return full[a].at[:, :, pl.ds(0, owners * count), cols]
        return full[a].at[pl.ds(0, count), :, pl.ds(0, owners * size), cols]

    one_side, both_sides = pl.ds(0, half), pl.ds(0, 2 * half)

    local = [pltpu.make_async_copy(own_shard(a), own_whole(a), local_sem.at[a]) for a in range(6)]
    features = [
        pltpu.make_async_copy(src, dst, local_sem.at[6 + k])
        for k, (src, dst) in enumerate(((s4, v4), (s3, v3)))
    ]
    bias_rows = [
        pltpu.make_async_copy(src, bias.at[pl.ds(k, 1), :], local_sem.at[8 + k])
        for k, src in enumerate((hb3, hb4, hb5, hc3, hc4, hc5))
    ]
    load5 = [
        pltpu.make_async_copy(s5.at[:, pl.ds(0, v5.shape[2])], v5.at[q], local_sem.at[14 + q])
        for q in range(v5.shape[0])
    ]
    lb3, lb4, lb5, ob3, ob4, ob5 = (bias.at[pl.ds(k, 1), :] for k in range(6))
    for copy in local:
        copy.start()
    if halved:
        for q in range(2):
            for owner in range(n):
                pltpu.make_async_copy(
                    s5.at[:, pl.ds((2 * owner + q) * parts[L5], parts[L5])],
                    v5.at[q, :, pl.ds(owner * parts[L5], parts[L5])],
                    local_sem.at[14 + q],
                ).start()
    else:
        load5[0].start()
    for copy in features + bias_rows:
        copy.start()

    zero5 = jnp.zeros((wid5, m5.shape[1]), BF16)
    m5[pl.ds(0, wid5), :] = zero5
    m5[pl.ds(m5.shape[0] - wid5, wid5), :] = zero5
    with jax.named_scope("meet"):
        pl.semaphore_wait(barrier, len(friends))

    def remote(src, dst, send, recv, device):
        return pltpu.make_async_remote_copy(
            src_ref=src, dst_ref=dst, send_sem=send, recv_sem=recv,
            device_id=device, device_id_type=pl.DeviceIdType.MESH,
        )

    def send(a, k, step, owner):
        if step <= hops[k]:
            spot = ring_part(a, owner)
            remote(spot, spot, sent.at[a], ring_recv.at[a, k * hops[0] + step - 1], target[k]).start()

    def cross(a, spot):
        remote(spot, spot, sent.at[a], core_recv.at[a], partner).start()

    def push(a):
        local[a].wait()
        for k in range(2):
            send(a, k, 1, s)

    def pull(a, k, step):
        owner = ring_owner(place - turn[k] * step, n)
        spot = ring_part(a, owner)
        sem = ring_recv.at[a, k * hops[0] + step - 1]
        remote(spot, spot, sent.at[a], sem, target[k]).wait_recv()
        send(a, k, step + 1, owner)
        if lent[a]:
            gift = mate_part(a, owner, plane)
            remote(gift, gift, sent.at[a], mate_recv.at[a, step - 1], mate).start()
        cross(a, spot)

    def accept(a, step):
        both = [k for k in range(2) if step <= hops[k]]
        spot = bulk(a, lent[a], len(both), one_side)
        remote(spot, spot, sent.at[a], mate_recv.at[a, step - 1], mate).wait_recv()
        for k in both:
            owner = ring_owner(place - turn[k] * step, n)
            cross(a, mate_part(a, owner, 1 - plane))

    def settle(a):
        spot = bulk(a, parts[a], n - 1, one_side)
        remote(spot, spot, sent.at[a], core_recv.at[a], partner).wait_recv()

    def drain(arrays):
        for a in arrays:
            spot = bulk(a, parts[a], n - 1, both_sides)
            remote(spot, spot, sent.at[a], core_recv.at[a], partner).wait_send()

    def map_rows(owner):
        count = rows5 * wid5
        return m5.at[pl.ds(pl.multiple_of(wid5 + owner * count, 16), count), :]

    across = s + 1 - 2 * (s % 2)

    def line_copy(j, owner):
        spot = map_rows(owner)
        peer = (dp, (s + 2 * j) % n)
        return remote(spot, spot, map_sent, line_recv.at[j - 1], peer)

    def pair_copy(owner):
        spot = map_rows(owner)
        return remote(spot, spot, map_sent, pair_recv, (dp, across))

    def map_view(count):
        return m5.at[pl.ds(0, count * rows5 * wid5), :]

    def line_pull(j):
        owner = (s + n - 2 * j) % n
        line_copy(j, owner).wait_recv()
        pair_copy(owner).start()

    if halved:
        swap = remote(v5.at[1 - plane], v5_mate, swap_sent, swap_recv.at[0], mate)
        partial = remote(out5, in5, partial_sent, swap_recv.at[1], mate)

    def half_five():
        settle(L5)
        swap.wait_recv()
        rows = jnp.concatenate([v5[plane], v5_mate[...]], axis=0)
        sums = jnp.dot(rows, w_l5[...], preferred_element_type=F32)
        own5[...] = sums[: own5.shape[0]]
        out5[...] = sums[own5.shape[0] :].astype(BF16)
        partial.start()

    here = pl.multiple_of(wid5 + s * (rows5 * wid5), 16)
    halos = []
    for k, (frame, rows, wid) in enumerate(((m4, rows4, wid4), (m3, rows3, wid3))):
        first, last = frame.at[pl.ds(wid, wid), :], frame.at[pl.ds(rows * wid, wid), :]
        top, bottom = frame.at[pl.ds(0, wid), :], frame.at[pl.ds((rows + 1) * wid, wid), :]
        halos.append((
            remote(last, top, halo_send.at[2 * k], halo_recv.at[2 * k], below),
            remote(first, bottom, halo_send.at[2 * k + 1], halo_recv.at[2 * k + 1], above),
        ))

    def start_halo(pair):
        @pl.when(s < n - 1)
        def _():
            pair[0].start()

        @pl.when(s > 0)
        def _():
            pair[1].start()

    def end_halo(pair, frame, rows, wid):
        @pl.when(s > 0)
        def _():
            pair[0].wait_recv()
            pair[1].wait_send()

        @pl.when(s < n - 1)
        def _():
            pair[1].wait_recv()
            pair[0].wait_send()

        zero = jnp.zeros((wid, frame.shape[1]), BF16)

        @pl.when(s == 0)
        def _():
            frame[pl.ds(0, wid), :] = zero

        @pl.when(s == n - 1)
        def _():
            frame[pl.ds((rows + 1) * wid, wid), :] = zero

    def prepare(level):
        if level == 4:
            settle(L4)
            features[0].wait()
            part4[...] = jnp.dot(v4[...], w_l4[...], preferred_element_type=F32) + lb4[...]
            return
        settle(L3)
        features[1].wait()
        tall = 2 * wid3

        def tile(i, carry):
            span = pl.ds(pl.multiple_of(i * tall, tall), tall)
            part3[span, :] = (
                jnp.dot(v3[span, :], w_l3[...], preferred_element_type=F32) + lb3[...]
            )
            return carry

        lax.fori_loop(0, rows4, tile, 0)

    def add_row(r, coarse, fine, part, wid):
        up = spread(coarse[pl.ds(pl.multiple_of(wid + r * wid, 16), wid), :])
        base = pl.multiple_of(4 * r * wid, 16)
        fine[pl.ds(pl.multiple_of(2 * wid + base, 16), 4 * wid), :] = (
            part[pl.ds(base, 4 * wid), :] + jnp.concatenate([up, up], axis=0)
        ).astype(BF16)

    def merge(level):
        if level == 5:
            if halved:
                partial.wait_recv()
                sums = own5[...] + in5[...].astype(F32)
            else:
                settle(L5)
                sums = jnp.dot(v5[0], w_l5[...], preferred_element_type=F32)
            m5[pl.ds(here, rows5 * wid5), :] = (sums + lb5[...]).astype(BF16)
            for j in range(1, n // 2):
                line_copy(j, s).start()
            pair_copy(s).start()
        elif level == 4:
            own_five = m5.at[pl.ds(pl.multiple_of(here - wid5, 16), (rows5 + 1) * wid5), :]
            for r in range(rows5):
                add_row(r, own_five, m4, part4, wid5)
            start_halo(halos[0])
        else:
            for r in sorted({0, rows4 - 1}):
                add_row(r, m4, m3, part3, wid4)
            start_halo(halos[1])

    def rest():
        def row(r, carry):
            add_row(r, m4, m3, part3, wid4)
            return carry

        lax.fori_loop(1, rows4 - 1, row, 0)

    def smooth(level):
        if level == 3:
            settle(O3)
            end_halo(halos[1], m3, rows3, wid3)
            conv(m3, w_o3, ob3, r3, rows3, wid3, 4)
            return
        if level == 4:
            settle(O4)
            end_halo(halos[0], m4, rows4, wid4)
            conv(m4, w_o4, ob4, r4, rows4, wid4, rows4)
            return
        settle(O5)
        spot = map_view(n // 2)
        remote(spot, spot, map_sent, pair_recv, (dp, across)).wait_recv()
        conv(m5, w_o5, ob5, r5, n * rows5, wid5, 16)
        few, many = r6.shape[0], r5.shape[0]
        pixel = lax.broadcasted_iota(jnp.int32, (few, many), 0)
        take = 2 * wid5 * (pixel // (wid5 // 2)) + 2 * (pixel % (wid5 // 2))
        pick = (take == lax.broadcasted_iota(jnp.int32, (few, many), 1)).astype(BF16)
        r6[...] = jnp.dot(pick, r5[...], preferred_element_type=F32).astype(BF16)

    def start_swap():
        for copy in load5 + bias_rows:
            copy.wait()
        if halved:
            swap.start()

    def handle(kind, a, k, step):
        if kind == PUSH:
            push(a)
        elif kind == PULL:
            pull(a, k, step)
        elif kind == MATE:
            accept(a, step)
        elif kind == SWAP:
            start_swap()
        elif kind == HALF:
            half_five()
        elif kind == PRE:
            prepare(a)
        elif kind == MERGE:
            merge(a)
        elif kind == REST:
            rest()
        elif kind == LINE:
            line_pull(a)
        else:
            smooth(a)

    def drain_maps():
        spot = map_view(n - 1)
        remote(spot, spot, map_sent, pair_recv, (dp, across)).wait_send()
        if halved:
            swap.wait_send()
            partial.wait_send()

    for event in schedule(hops, lent, halved, n // 2):
        if event[:2] == (CONV, 5):
            drain((L5, L4, L3))
        with jax.named_scope("_".join(map(str, event))):
            handle(*event)

    with jax.named_scope("drain_maps"):
        drain_maps()
    with jax.named_scope("last"):
        smooth(4)
    with jax.named_scope("drain"):
        drain((O3, O5, O4))


def finish(*refs):
    results, outputs, sems = refs[:4], refs[4:8], refs[8]
    copies = [
        pltpu.make_async_copy(src, dst, sems.at[k])
        for k, (src, dst) in enumerate(zip(results, outputs))
    ]
    for copy in copies:
        copy.start()
    for copy in copies:
        copy.wait()


def on_device(n, dps, *arrays):
    s3, s4, s5, l3, l4, l5, lb3, lb4, lb5, o3, o4, o5, ob3, ob4, ob5 = arrays
    dims = tuple(x.shape[1:3] for x in (s3, s4, s5))
    fd = l3.shape[1]
    (rows3, wid3), (rows4, wid4), (rows5, wid5) = dims
    flat = [x.reshape(-1, x.shape[3]) for x in (s3, s4, s5)]
    biases = [b.reshape(1, fd) for b in (lb3, lb4, lb5, ob3, ob4, ob5)]
    anywhere = pl.BlockSpec(memory_space=pl.ANY)
    near = pl.BlockSpec(memory_space=pltpu.VMEM)
    far = max(n // 2, 1)
    size5, wide5 = flat[2].shape
    deep5 = l5.shape[0]
    halved = dps % 4 == 0 and deep5 % 256 == 0
    split5 = 2 if halved else 1

    def array(*shape):
        return pltpu.VMEM(shape, BF16)

    def result(pixels):
        return jax.ShapeDtypeStruct((pixels, fd), BF16)

    dma = pltpu.SemaphoreType.DMA
    held = pl.pallas_call(
        functools.partial(kernel, n, dims, dps),
        out_shape=(
            array(rows3 * wid3, fd),
            array(rows4 * wid4, fd),
            array(n * rows5 * wid5, fd),
            array(n * rows5 * wid5 // 4, fd),
        ),
        in_specs=[anywhere] * 15,
        out_specs=(near,) * 4,
        scratch_shapes=[
            *(array(*x.shape) for x in flat[:2]),
            array(split5, size5, wide5 // split5),
            array(size5, wide5 // split5),
            pltpu.VMEM((size5, fd), F32),
            *(array(size5, fd) for _ in range(2)),
            array(n * deep5 // split5, fd),
            array(n * l4.shape[0], fd),
            array(n * l3.shape[0], fd),
            *(array(3, 3, n * x.shape[2], fd) for x in (o3, o5, o4)),
            array((rows3 + 2) * wid3, fd),
            array((rows4 + 2) * wid4, fd),
            array((n * rows5 + 2) * wid5, fd),
            pltpu.VMEM((rows3 * wid3, fd), F32),
            pltpu.VMEM((rows4 * wid4, fd), F32),
            pltpu.VMEM((6, fd), F32),
            dma((6,)),
            dma((6, n - 1)),
            dma((6, far)),
            dma((6,)),
            dma,
            dma((far,)),
            dma,
            dma,
            dma,
            dma((2,)),
            dma((4,)),
            dma((4,)),
            dma((16,)),
        ],
        compiler_params=pltpu.CompilerParams(
            collective_id=0, has_side_effects=True, vmem_limit_bytes=40 * 1024 * 1024
        ),
    )(*[
        pltpu.with_memory_space_constraint(x, pltpu.HBM)
        for x in (*flat, l3, l4, l5, *biases[:3], o3, o4, o5, *biases[3:])
    ])
    y3, y4, y5, y6 = pl.pallas_call(
        finish,
        out_shape=(
            result(rows3 * wid3),
            result(rows4 * wid4),
            result(n * rows5 * wid5),
            result(n * rows5 * wid5 // 4),
        ),
        in_specs=[near] * 4,
        out_specs=(anywhere,) * 4,
        scratch_shapes=[dma((4,))],
        compiler_params=pltpu.CompilerParams(vmem_limit_bytes=32 * 1024 * 1024),
    )(*[pltpu.with_memory_space_constraint(x, pltpu.VMEM) for x in held])
    return (
        y3.reshape(1, rows3, wid3, fd),
        y4.reshape(1, rows4, wid4, fd),
        y5.reshape(1, n * rows5, wid5, fd),
        y6.reshape(1, n * rows5 // 2, wid5 // 2, fd),
    )


def solution(mesh):
    split, rows = P("dp", "space", None, None), P("space", None)
    taps = P(None, None, "space", None)
    whole = P("dp", None, None, None)
    return jax.shard_map(
        functools.partial(on_device, mesh.shape["space"], mesh.shape["dp"]),
        mesh=mesh,
        in_specs=(split,) * 3 + (rows,) * 3 + (P(),) * 3 + (taps,) * 3 + (P(),) * 3,
        out_specs=(split, split, whole, whole),
        check_vma=False,
    )
```
